32 devices in a mesh: group: 2 (over y), seq: 4 (over z), tensor: 4 (over x, core).
Axes of the slice: x: 2, y: 2, z: 4, core: 2. Of those that a mesh axis runs over, the one named last changes fastest.
Arguments:
- query: bfloat16 [16, 7168], P(('group', 'seq'), 'tensor'), parts along dimension 0, may hold values from -5 to 5
- key_cache: bfloat16 [32, 256, 7168], P(('group', 'seq'), None, 'tensor'), parts along dimension 0, may hold values from -5 to 5
- value_cache: bfloat16 [32, 256, 7168], P(('group', 'seq'), None, 'tensor'), parts along dimension 0, may hold values from -6 to 6
- alibi_slopes: float32 [56], P('tensor'), may hold values from 0 to 1, as said below
- block_seq: int32 [32], P(('group', 'seq')), parts along dimension 0, may hold values from 0 to 7, as said below
- block_pos: int32 [32], P(('group', 'seq')), parts along dimension 0, may hold values from 0 to 2, as said below
- lengths: int32 [16], P('group'), parts along dimension 0, may hold values from 1 to 768, as said below
- out_weight: bfloat16 [7168, 14336], P('tensor', 'seq'), may hold values from -0.5 to 0.5
Outputs:
- mixed: bfloat16 [16, 14336], P(('group', 'tensor'), 'seq'), parts along dimension 0
The draws below stay inside these ranges and needn't reach their ends.
There are 2 independent parts, one for each index of `group`. The reference program is written for one: setup_inputs(seed, part) draws one part's arguments, and reference() takes and returns one part's arrays. A program takes and returns all parts, laid end to end along the dimension named above; an argument that names none is the same for every part. Nothing has to cross between parts.
Inputs may be any that keep to these rules, and one draw needn't show every extreme that they name: `block_seq`: every sequence owns at least one block and at most 3; the blocks of sequence s have block_pos 0 to n_s - 1, each once. block_pos of a block is below the number of blocks its sequence owns. `lengths`: A sequence that owns n blocks has a length above 256 * (n - 1) and at most 256 * n. `alibi_slopes`: positive slopes.
All inputs are finite; a program needn't handle non-finite values.
Results may differ from the reference program's by a relative error of at most 0.0054.
Values may be sent and summed in bfloat16 or wider, within the bound.
A program may use at most 64 MiB of HBM per device.

```python
import math
import jax
import jax.numpy as jnp
from jax import lax

D = 14336
HEADS = 56
HEAD_DIM = 128
BLOCK = 256
SEQS = 8
BLOCKS = 16
MOST_BLOCKS = 3


def block_layout(key):
    second = jax.random.fold_in(key, 12)
    third = jax.random.fold_in(key, 13)
    fourth = jax.random.fold_in(key, 14)
    fifth = jax.random.fold_in(key, 15)
    extra = BLOCKS - SEQS
    capacity = MOST_BLOCKS - 1
    remain = extra - capacity
    relabel = jax.random.permutation(third, SEQS).astype(jnp.int32)
    longest = relabel[0]
    seq_ids = jnp.arange(SEQS, dtype=jnp.int32)
    counts = 1 + capacity * (seq_ids == longest).astype(jnp.int32)
    if remain > 0:
        order = jax.random.permutation(second, (SEQS - 1) * capacity)[:remain].astype(jnp.int32)
        target = relabel[1 + order // capacity]
        counts = counts + jnp.sum((target[:, None] == seq_ids[None, :]).astype(jnp.int32), axis=0)
    ends = jnp.cumsum(counts).astype(jnp.int32)
    starts = ends - counts
    slots = jnp.arange(BLOCKS, dtype=jnp.int32)
    seq_of = jnp.sum((ends[None, :] <= slots[:, None]).astype(jnp.int32), axis=1)
    pos_of = slots - starts[seq_of]
    placed = jax.random.permutation(fourth, BLOCKS)
    owners = jnp.zeros((BLOCKS,), jnp.int32).at[placed].set(seq_of)
    places = jnp.zeros((BLOCKS,), jnp.int32).at[placed].set(pos_of)
    tails = jax.random.randint(fifth, (SEQS,), 1, BLOCK + 1).astype(jnp.int32)
    tails = jnp.where(seq_ids == longest, BLOCK, tails)
    sizes_out = ((counts - 1) * BLOCK + tails).astype(jnp.int32)
    return (owners, places, sizes_out)


def draw_block_seq(key, part):
    return block_layout(key)[0]


def draw_block_pos(key, part):
    return block_layout(key)[1]


def draw_lengths(key, part):
    return block_layout(key)[2]


def draw_query(key, part):
    base = jnp.clip(jax.random.normal(jax.random.fold_in(key, 21), (SEQS, HEADS, HEAD_DIM), jnp.float32), -5.0, 5.0)
    return base.reshape(SEQS, HEADS * HEAD_DIM).astype(jnp.bfloat16)


def draw_key_cache(key, part):
    base = jnp.clip(jax.random.normal(jax.random.fold_in(key, 23), (BLOCKS, BLOCK, HEADS * HEAD_DIM), jnp.float32), -5.0, 5.0)
    return base.astype(jnp.bfloat16)


def draw_alibi_slopes(key, part):
    spread = jax.random.uniform(jax.random.fold_in(key, 32), (HEADS,), jnp.float32)
    strong = jax.random.randint(jax.random.fold_in(key, 31), (HEADS,), 0, 2) == 1
    slow = jnp.exp(jnp.log(1.0 / 8192.0) + spread * jnp.log(8.0))
    fast = jnp.exp(jnp.log(1.0 / 64.0) + spread * jnp.log(8.0))
    return jnp.where(strong, fast, slow).astype(jnp.float32)


def steps_of(rng, shape, shards, least, high):
    factor_of, own = 1.0, jax.random.fold_in(rng, 6)
    for axis_at, parts in shards:
        steps = jnp.exp(jax.random.uniform(jax.random.fold_in(own, axis_at), (parts,), jnp.float32, least / len(shards), high / len(shards)))
        factor_of = factor_of * jnp.repeat(steps, shape[axis_at] // parts).reshape([-1 if axis == axis_at else 1 for axis in range(len(shape))])
    return factor_of


def scatter_about(rng, extent, deviation, bound, split=(), kind=jnp.bfloat16):
    array = jax.random.normal(rng, extent, jnp.float32) * deviation
    if len(split) > 0:
        array = steps_of(rng, extent, split, -0.22, 0.18) * array
    return jnp.clip(array, min=-bound, max=bound).astype(kind)


def setup_inputs(seed: int = 0, part: int = 0) -> dict:
    streams_of = jax.random.split(jax.random.key(seed), 9)
    part_keys = jax.random.split(jax.random.fold_in(streams_of[8], part), 9)
    return {
        "query": draw_query(jax.random.fold_in(jax.random.fold_in(streams_of[8], part), 71), part),
        "key_cache": draw_key_cache(jax.random.fold_in(jax.random.fold_in(streams_of[8], part), 71), part),
        "value_cache": scatter_about(part_keys[2], (BLOCKS, BLOCK, HEADS * HEAD_DIM), 1.0, 6.0, ((0, 4), (2, 4))),
        "alibi_slopes": draw_alibi_slopes(jax.random.fold_in(streams_of[8], 71), part),
        "block_seq": draw_block_seq(jax.random.fold_in(jax.random.fold_in(streams_of[8], part), 71), part),
        "block_pos": draw_block_pos(jax.random.fold_in(jax.random.fold_in(streams_of[8], part), 71), part),
        "lengths": draw_lengths(jax.random.fold_in(jax.random.fold_in(streams_of[8], part), 71), part),
        "out_weight": scatter_about(streams_of[7], (HEADS * HEAD_DIM, D), HEAD_DIM ** -0.5, 0.5, ((0, 4), (1, 4))),
    }


def reference(query, key_cache, value_cache, alibi_slopes, block_seq, block_pos, lengths, out_weight):
    scale = 1.0 / math.sqrt(HEAD_DIM)
    offsets = jnp.arange(BLOCK, dtype=jnp.int32)

    def one_block(index):
        owner = block_seq[index]
        length = lengths[owner]
        placed = block_pos[index] * BLOCK + offsets
        live = placed < length
        qrow = query[owner].astype(jnp.float32).reshape(HEADS, HEAD_DIM)
        keys = key_cache[index].astype(jnp.float32).reshape(BLOCK, HEADS, HEAD_DIM)
        values = value_cache[index].astype(jnp.float32).reshape(BLOCK, HEADS, HEAD_DIM)
        scores = jnp.einsum('thd,hd->ht', keys, qrow) * scale
        distance = (length - 1 - placed).astype(jnp.float32)
        scores = scores - alibi_slopes[:, None] * distance[None, :]
        scores = jnp.where(live[None, :], scores, -1e+30)
        top = lax.optimization_barrier(jnp.max(scores, axis=1))
        weights = jnp.where(live[None, :], jnp.exp(scores - top[:, None]), 0.0)
        total = lax.optimization_barrier(jnp.sum(weights, axis=1))
        rounded = lax.optimization_barrier(weights.astype(jnp.bfloat16)).astype(jnp.float32)
        summed = jnp.einsum('ht,thd->hd', rounded, values)
        return (top, total, summed)
    tops, totals, sums = lax.map(one_block, jnp.arange(BLOCKS, dtype=jnp.int32))
    seq_ids = jnp.arange(SEQS, dtype=jnp.int32)
    owned = block_seq[None, :] == seq_ids[:, None]
    seq_max = lax.optimization_barrier(jnp.max(jnp.where(owned[:, :, None], tops[None], -1e+30), axis=1))
    factor = jnp.where(owned[:, :, None], jnp.exp(tops[None] - seq_max[:, None, :]), 0.0)
    seq_sum = lax.optimization_barrier(jnp.sum(factor * totals[None], axis=1))
    seq_acc = jnp.einsum('sbh,bhd->shd', factor, sums, precision=lax.Precision.HIGHEST)
    attention = (seq_acc / seq_sum[:, :, None]).reshape(SEQS, HEADS * HEAD_DIM).astype(jnp.bfloat16)
    return jnp.dot(attention, out_weight, preferred_element_type=jnp.float32).astype(jnp.bfloat16)
```

```python
import functools
import math

import jax
import jax.numpy as jnp
from jax import lax
from jax.experimental import pallas as pl
from jax.experimental.pallas import tpu as pltpu
from jax.sharding import PartitionSpec as P

LANES = 128
OWNER_LANE = LANES - 1


def kernel(
    seq_size, tensor_size, heads, chunks,
    block_seq, block_pos, lengths, slopes, query, keys, values, weight,
    out,
    q_all, k_buf, v_buf, w_buf, stats, accs, part, landed,
    q_sem, k_sem, v_sem, w_sem,
    q_send, q_recv, s_send, s_recv, a_send, a_recv, p_send, p_recv,
):
    me = lax.axis_index("seq")
    my_rows = lax.axis_index("tensor")
    blocks, block_len, features = k_buf.shape
    size = features // heads
    padded = -(-heads // 16) * 16
    seqs = lengths.shape[0]
    query_rows = q_all.shape[1]
    rows, width = part.shape[2:]
    scale = 1.0 / math.sqrt(size)

    q_copy = pltpu.make_async_copy(query, q_all.at[me], q_sem)
    q_copy.start()
    k_copies = [
        pltpu.make_async_copy(keys.at[b], k_buf.at[b], k_sem.at[b]) for b in range(blocks)
    ]
    v_copies = [
        pltpu.make_async_copy(values.at[b], v_buf.at[b], v_sem.at[b]) for b in range(blocks)
    ]
    w_copies = [
        pltpu.make_async_copy(
            weight.at[:, pl.ds(c * width, width)],
            w_buf.at[:, pl.ds(c * width, width)],
            w_sem.at[c],
        )
        for c in range(chunks)
    ]
    for copy in k_copies + v_copies + w_copies:
        copy.start()

    barrier = pltpu.get_barrier_semaphore()
    for k in range(1, seq_size):
        pl.semaphore_signal(barrier, inc=1, device_id={"seq": lax.rem(me + k, seq_size)})
    for k in range(1, tensor_size):
        pl.semaphore_signal(
            barrier, inc=1, device_id={"tensor": lax.rem(my_rows + k, tensor_size)}
        )
    pl.semaphore_wait(barrier, seq_size + tensor_size - 2)

    def to_seq(buffer, send, recv):
        copies = [
            pltpu.make_async_remote_copy(
                src_ref=buffer.at[me],
                dst_ref=buffer.at[me],
                send_sem=send.at[k - 1],
                recv_sem=recv.at[k - 1],
                device_id={"seq": lax.rem(me + k, seq_size)},
            )
            for k in range(1, seq_size)
        ]
        for copy in copies:
            copy.start()
        return copies

    q_copy.wait()
    q_sends = to_seq(q_all, q_send, q_recv)

    lane = lax.broadcasted_iota(jnp.int32, (padded, features), 1)
    row = lax.broadcasted_iota(jnp.int32, (padded, features), 0)
    of_head = (lane >= row * size) & (lane < row * size + size)
    head_row = lax.broadcasted_iota(jnp.int32, (padded, LANES), 0)
    head_lane = lax.broadcasted_iota(jnp.int32, (padded, LANES), 1)
    slope = jnp.zeros((padded, LANES), jnp.float32)
    for h in range(heads):
        slope = jnp.where(head_row == h, slopes[h], slope)
    slope = slope[:, :1]
    offsets = lax.broadcasted_iota(jnp.int32, (1, block_len), 1)
    stat_lane = lax.broadcasted_iota(jnp.int32, (1, LANES), 1)

    for copy in q_sends:
        copy.wait_recv()

    weights, inverse, stat_rows = [], [], []
    for b in range(blocks):
        owner = block_seq[b]
        length = lengths[owner]
        near = q_all[lax.div(owner, query_rows)].astype(jnp.float32)
        which = lax.rem(owner, query_rows)
        q_row = near[:1]
        for r in range(1, query_rows):
            q_row = jnp.where(which == r, near[r : r + 1], q_row)
        spread = jnp.where(of_head, q_row, 0.0).astype(jnp.bfloat16)
        k_copies[b].wait()
        scores = lax.dot_general(
            spread, k_buf[b], (((1,), (1,)), ((), ())), preferred_element_type=jnp.float32
        )
        placed = block_pos[b] * block_len + offsets
        live = placed < length
        distance = (length - 1 - placed).astype(jnp.float32)
        scores = jnp.where(live, scores * scale - slope * distance, -1e30)
        top = jnp.max(scores, axis=1, keepdims=True)
        weight_b = jnp.where(live, jnp.exp(scores - top), 0.0)
        total = jnp.sum(weight_b, axis=1, keepdims=True)
        weights.append(weight_b.astype(jnp.bfloat16))
        inverse.append(1.0 / total)
        stat = jnp.sum(
            jnp.where(head_row == head_lane, top + jnp.log(total), 0.0), axis=0, keepdims=True
        )
        stat_rows.append(jnp.where(stat_lane == OWNER_LANE, owner.astype(jnp.float32), stat))
    stats[me] = jnp.concatenate(stat_rows, axis=0)
    s_sends = to_seq(stats, s_send, s_recv)

    acc_rows = []
    for b in range(blocks):
        v_copies[b].wait()
        summed = jnp.dot(weights[b], v_buf[b], preferred_element_type=jnp.float32)
        summed = summed * inverse[b]
        acc_rows.append(
            jnp.sum(jnp.where(of_head, summed, 0.0), axis=0, keepdims=True)
        )
    accs[me] = jnp.concatenate(acc_rows, axis=0).astype(jnp.bfloat16)
    a_sends = to_seq(accs, a_send, a_recv)

    for copy in s_sends:
        copy.wait_recv()
    stat = stats[...]
    owners = stat[:, :, OWNER_LANE:]
    best = jnp.zeros_like(stat)
    masks = [owners == float(s) for s in range(seqs)]
    for s in range(seqs):
        top = jnp.max(jnp.where(masks[s], stat, -1e30), axis=(0, 1), keepdims=True)
        best = jnp.where(masks[s], top, best)
    grown = jnp.exp(stat - best)
    whole = jnp.ones_like(stat)
    for s in range(seqs):
        total = jnp.sum(jnp.where(masks[s], grown, 0.0), axis=(0, 1), keepdims=True)
        whole = jnp.where(masks[s], total, whole)
    factor = grown / whole
    seq_lane = lax.broadcasted_iota(jnp.int32, (blocks, LANES), 1).astype(jnp.float32)
    owned = jnp.concatenate(
        [jnp.where(owners[j] == seq_lane, 1.0, 0.0) for j in range(seq_size)], axis=0
    )
    owned = owned.T[:seqs].astype(jnp.bfloat16)
    spread = [
        jnp.concatenate(
            [jnp.broadcast_to(factor[j][:, h : h + 1], (blocks, size)) for h in range(heads)],
            axis=1,
        )
        for j in range(seq_size)
    ]

    for copy in a_sends:
        copy.wait_recv()
    scaled = jnp.concatenate(
        [accs[j].astype(jnp.float32) * spread[j] for j in range(seq_size)], axis=0
    )
    high = scaled.astype(jnp.bfloat16)
    low = (scaled - high.astype(jnp.float32)).astype(jnp.bfloat16)
    attention = jnp.dot(owned, high, preferred_element_type=jnp.float32) + jnp.dot(
        owned, low, preferred_element_type=jnp.float32
    )
    attention = attention.astype(jnp.bfloat16)

    p_sends = []
    for c in range(chunks):
        w_copies[c].wait()
        product = jnp.dot(
            attention, w_buf[:, c * width : (c + 1) * width], preferred_element_type=jnp.float32
        )
        for r in range(tensor_size):
            part[r, c] = product[r * rows : (r + 1) * rows]
        sends = []
        for k in range(1, tensor_size):
            peer = lax.rem(my_rows + k, tensor_size)
            copy = pltpu.make_async_remote_copy(
                src_ref=part.at[peer, c],
                dst_ref=landed.at[k - 1, c],
                send_sem=p_send.at[k - 1, c],
                recv_sem=p_recv.at[k - 1, c],
                device_id={"tensor": peer},
            )
            copy.start()
            sends.append(copy)
        p_sends.append(sends)
    for c in range(chunks):
        total = part[my_rows, c]
        for k in range(1, tensor_size):
            p_sends[c][k - 1].wait_recv()
            total = total + landed[k - 1, c]
        out[:, c * width : (c + 1) * width] = total.astype(out.dtype)
    for copy in q_sends + s_sends + a_sends + [copy for sends in p_sends for copy in sends]:
        copy.wait_send()


def local(seq_size, tensor_size, query, key_cache, value_cache, slopes, block_seq, block_pos, lengths, weight):
    heads = slopes.shape[0]
    blocks, block_len, features = key_cache.shape
    columns = weight.shape[1]
    chunks = max([c for c in range(1, 9) if columns % (c * 256) == 0], default=1)
    width = columns // chunks
    rows = lengths.shape[0] // tensor_size
    smem = pl.BlockSpec(memory_space=pltpu.SMEM)
    anywhere = pl.BlockSpec(memory_space=pl.ANY)
    dma = pltpu.SemaphoreType.DMA
    return pl.pallas_call(
        functools.partial(kernel, seq_size, tensor_size, heads, chunks),
        out_shape=jax.ShapeDtypeStruct((rows, columns), jnp.bfloat16),
        in_specs=[smem] * 4 + [anywhere] * 4,
        out_specs=pl.BlockSpec(memory_space=pltpu.VMEM),
        scratch_shapes=[
            pltpu.VMEM((seq_size,) + query.shape, query.dtype),
            pltpu.VMEM(key_cache.shape, key_cache.dtype),
            pltpu.VMEM(value_cache.shape, value_cache.dtype),
            pltpu.VMEM(weight.shape, weight.dtype),
            pltpu.VMEM((seq_size, blocks, LANES), jnp.float32),
            pltpu.VMEM((seq_size, blocks, features), jnp.bfloat16),
            pltpu.VMEM((tensor_size, chunks, rows, width), jnp.float32),
            pltpu.VMEM((tensor_size - 1, chunks, rows, width), jnp.float32),
            dma,
            dma((blocks,)),
            dma((blocks,)),
            dma((chunks,)),
        ]
        + [dma((seq_size - 1,))] * 6
        + [dma((tensor_size - 1, chunks))] * 2,
        compiler_params=pltpu.CompilerParams(collective_id=0, has_side_effects=True),
    )(block_seq, block_pos, lengths, slopes, query, key_cache, value_cache, weight)


def solution(mesh):
    placed = (
        P(("group", "seq"), "tensor"),
        P(("group", "seq"), None, "tensor"),
        P(("group", "seq"), None, "tensor"),
        P("tensor"),
        P(("group", "seq")),
        P(("group", "seq")),
        P("group"),
        P("tensor", "seq"),
    )
    return jax.shard_map(
        functools.partial(local, mesh.shape["seq"], mesh.shape["tensor"]),
        mesh=mesh,
        in_specs=placed,
        out_specs=P(("group", "tensor"), "seq"),
        check_vma=False,
    )
```

```python
import functools
import math

import jax
import jax.numpy as jnp
from jax import lax
from jax.experimental import pallas as pl
from jax.experimental.pallas import tpu as pltpu
from jax.sharding import PartitionSpec as P

LANES = 128
OWNER_LANE = LANES - 1


def kernel(
    seq_size, tensor_size, heads, chunks,
    block_seq, block_pos, lengths, slopes, query, keys, values, weight,
    out,
    q_all, k_buf, v_buf, w_buf, stats, accs, part, landed,
    q_sem, k_sem, v_sem, w_sem,
    q_send, q_recv, s_send, s_recv, a_send, a_recv, p_send, p_recv,
):
    me = lax.axis_index("seq")
    my_rows = lax.axis_index("tensor")
    blocks, block_len, features = k_buf.shape
    size = features // heads
    padded = -(-heads // 16) * 16
    seqs = lengths.shape[0]
    query_rows = q_all.shape[1]
    rows, width = part.shape[2:]
    scale = 1.0 / math.sqrt(size)

    q_copy = pltpu.make_async_copy(query, q_all.at[me], q_sem)
    q_copy.start()
    k_copies = [
        pltpu.make_async_copy(keys.at[b], k_buf.at[b], k_sem.at[b]) for b in range(blocks)
    ]
    v_copies = [
        pltpu.make_async_copy(values.at[b], v_buf.at[b], v_sem.at[b]) for b in range(blocks)
    ]
    w_copies = [
        pltpu.make_async_copy(
            weight.at[:, pl.ds(c * width, width)],
            w_buf.at[:, pl.ds(c * width, width)],
            w_sem.at[c],
        )
        for c in range(chunks)
    ]
    barrier = pltpu.get_barrier_semaphore()
    for k in range(1, seq_size):
        pl.semaphore_signal(barrier, inc=1, device_id={"seq": lax.rem(me + k, seq_size)})
    for k in range(1, tensor_size):
        pl.semaphore_signal(
            barrier, inc=1, device_id={"tensor": lax.rem(my_rows + k, tensor_size)}
        )
    q_copy.wait()
    for copy in k_copies + v_copies:
        copy.start()
    pl.semaphore_wait(barrier, seq_size + tensor_size - 2)

    def to_seq(buffer, send, recv):
        copies = [
            pltpu.make_async_remote_copy(
                src_ref=buffer.at[me],
                dst_ref=buffer.at[me],
                send_sem=send.at[k - 1],
                recv_sem=recv.at[k - 1],
                device_id={"seq": lax.rem(me + k, seq_size)},
            )
            for k in range(1, seq_size)
        ]
        for copy in copies:
            copy.start()
        return copies

    q_sends = to_seq(q_all, q_send, q_recv)

    lane = lax.broadcasted_iota(jnp.int32, (padded, features), 1)
    row = lax.broadcasted_iota(jnp.int32, (padded, features), 0)
    of_head = (lane >= row * size) & (lane < row * size + size)
    head_row = lax.broadcasted_iota(jnp.int32, (padded, LANES), 0)
    head_lane = lax.broadcasted_iota(jnp.int32, (padded, LANES), 1)
    slope = jnp.zeros((padded, LANES), jnp.float32)
    for h in range(heads):
        slope = jnp.where(head_row == h, slopes[h], slope)
    slope = slope[:, :1]
    offsets = lax.broadcasted_iota(jnp.int32, (1, block_len), 1)
    stat_lane = lax.broadcasted_iota(jnp.int32, (1, LANES), 1)

    for copy in q_sends:
        copy.wait_recv()
    for copy in w_copies:
        copy.start()
    for copy in k_copies + v_copies:
        copy.wait()

    weights, inverse, stat_rows = [], [], []
    for b in range(blocks):
        owner = block_seq[b]
        length = lengths[owner]
        near = q_all[lax.div(owner, query_rows)].astype(jnp.float32)
        which = lax.rem(owner, query_rows)
        q_row = near[:1]
        for r in range(1, query_rows):
            q_row = jnp.where(which == r, near[r : r + 1], q_row)
        spread = jnp.where(of_head, q_row, 0.0).astype(jnp.bfloat16)
        scores = lax.dot_general(
            spread, k_buf[b], (((1,), (1,)), ((), ())), preferred_element_type=jnp.float32
        )
        placed = block_pos[b] * block_len + offsets
        live = placed < length
        distance = (length - 1 - placed).astype(jnp.float32)
        scores = jnp.where(live, scores * scale - slope * distance, -1e30)
        top = jnp.max(scores, axis=1, keepdims=True)
        weight_b = jnp.where(live, jnp.exp(scores - top), 0.0)
        total = jnp.sum(weight_b, axis=1, keepdims=True)
        weights.append(weight_b.astype(jnp.bfloat16))
        inverse.append(1.0 / total)
        stat = jnp.sum(
            jnp.where(head_row == head_lane, top + jnp.log(total), 0.0), axis=0, keepdims=True
        )
        stat_rows.append(jnp.where(stat_lane == OWNER_LANE, owner.astype(jnp.float32), stat))
    stats[me] = jnp.concatenate(stat_rows, axis=0)
    s_sends = to_seq(stats, s_send, s_recv)

    acc_rows = []
    for b in range(blocks):
        summed = jnp.dot(weights[b], v_buf[b], preferred_element_type=jnp.float32)
        summed = summed * inverse[b]
        acc_rows.append(
            jnp.sum(jnp.where(of_head, summed, 0.0), axis=0, keepdims=True)
        )
    accs[me] = jnp.concatenate(acc_rows, axis=0).astype(jnp.bfloat16)
    a_sends = to_seq(accs, a_send, a_recv)

    for copy in s_sends:
        copy.wait_recv()
    stat = stats[...]
    owners = stat[:, :, OWNER_LANE:]
    best = jnp.zeros_like(stat)
    masks = [owners == float(s) for s in range(seqs)]
    for s in range(seqs):
        top = jnp.max(jnp.where(masks[s], stat, -1e30), axis=(0, 1), keepdims=True)
        best = jnp.where(masks[s], top, best)
    grown = jnp.exp(stat - best)
    whole = jnp.ones_like(stat)
    for s in range(seqs):
        total = jnp.sum(jnp.where(masks[s], grown, 0.0), axis=(0, 1), keepdims=True)
        whole = jnp.where(masks[s], total, whole)
    factor = grown / whole
    seq_lane = lax.broadcasted_iota(jnp.int32, (blocks, LANES), 1).astype(jnp.float32)
    owned = jnp.concatenate(
        [jnp.where(owners[j] == seq_lane, 1.0, 0.0) for j in range(seq_size)], axis=0
    )
    owned = owned.T[:seqs].astype(jnp.bfloat16)
    spread = [
        jnp.concatenate(
            [jnp.broadcast_to(factor[j][:, h : h + 1], (blocks, size)) for h in range(heads)],
            axis=1,
        )
        for j in range(seq_size)
    ]

    for copy in a_sends:
        copy.wait_recv()
    scaled = jnp.concatenate(
        [accs[j].astype(jnp.float32) * spread[j] for j in range(seq_size)], axis=0
    )
    high = scaled.astype(jnp.bfloat16)
    low = (scaled - high.astype(jnp.float32)).astype(jnp.bfloat16)
    attention = jnp.dot(owned, high, preferred_element_type=jnp.float32) + jnp.dot(
        owned, low, preferred_element_type=jnp.float32
    )
    attention = attention.astype(jnp.bfloat16)

    p_sends = []
    for copy in w_copies:
        copy.wait()
    for c in range(chunks):
        product = jnp.dot(
            attention, w_buf[:, c * width : (c + 1) * width], preferred_element_type=jnp.float32
        )
        for r in range(tensor_size):
            part[r, c] = product[r * rows : (r + 1) * rows]
        sends = []
        for k in range(1, tensor_size):
            peer = lax.rem(my_rows + k, tensor_size)
            copy = pltpu.make_async_remote_copy(
                src_ref=part.at[peer, c],
                dst_ref=landed.at[k - 1, c],
                send_sem=p_send.at[k - 1, c],
                recv_sem=p_recv.at[k - 1, c],
                device_id={"tensor": peer},
            )
            copy.start()
            sends.append(copy)
        p_sends.append(sends)
    for c in range(chunks):
        total = part[my_rows, c]
        for k in range(1, tensor_size):
            p_sends[c][k - 1].wait_recv()
            total = total + landed[k - 1, c]
        out[:, c * width : (c + 1) * width] = total.astype(out.dtype)
    for copy in q_sends + s_sends + a_sends + [copy for sends in p_sends for copy in sends]:
        copy.wait_send()


def local(seq_size, tensor_size, query, key_cache, value_cache, slopes, block_seq, block_pos, lengths, weight):
    heads = slopes.shape[0]
    blocks, block_len, features = key_cache.shape
    columns = weight.shape[1]
    chunks = max([c for c in range(1, 9) if columns % (c * 256) == 0], default=1)
    width = columns // chunks
    rows = lengths.shape[0] // tensor_size
    smem = pl.BlockSpec(memory_space=pltpu.SMEM)
    anywhere = pl.BlockSpec(memory_space=pl.ANY)
    dma = pltpu.SemaphoreType.DMA
    return pl.pallas_call(
        functools.partial(kernel, seq_size, tensor_size, heads, chunks),
        out_shape=jax.ShapeDtypeStruct((rows, columns), jnp.bfloat16),
        in_specs=[smem] * 4 + [anywhere] * 4,
        out_specs=pl.BlockSpec(memory_space=pltpu.VMEM),
        scratch_shapes=[
            pltpu.VMEM((seq_size,) + query.shape, query.dtype),
            pltpu.VMEM(key_cache.shape, key_cache.dtype),
            pltpu.VMEM(value_cache.shape, value_cache.dtype),
            pltpu.VMEM(weight.shape, weight.dtype),
            pltpu.VMEM((seq_size, blocks, LANES), jnp.float32),
            pltpu.VMEM((seq_size, blocks, features), jnp.bfloat16),
            pltpu.VMEM((tensor_size, chunks, rows, width), jnp.float32),
            pltpu.VMEM((tensor_size - 1, chunks, rows, width), jnp.float32),
            dma,
            dma((blocks,)),
            dma((blocks,)),
            dma((chunks,)),
        ]
        + [dma((seq_size - 1,))] * 6
        + [dma((tensor_size - 1, chunks))] * 2,
        compiler_params=pltpu.CompilerParams(collective_id=0, has_side_effects=True),
    )(block_seq, block_pos, lengths, slopes, query, key_cache, value_cache, weight)


def solution(mesh):
    placed = (
        P(("group", "seq"), "tensor"),
        P(("group", "seq"), None, "tensor"),
        P(("group", "seq"), None, "tensor"),
        P("tensor"),
        P(("group", "seq")),
        P(("group", "seq")),
        P("group"),
        P("tensor", "seq"),
    )
    return jax.shard_map(
        functools.partial(local, mesh.shape["seq"], mesh.shape["tensor"]),
        mesh=mesh,
        in_specs=placed,
        out_specs=P(("group", "tensor"), "seq"),
        check_vma=False,
    )
```

```python
import functools
import math

import jax
import jax.numpy as jnp
from jax import lax
from jax.experimental import pallas as pl
from jax.experimental.pallas import tpu as pltpu
from jax.sharding import PartitionSpec as P

LANES = 128
OWNER_LANE = LANES - 1


def kernel(
    seq_size, tensor_size, groups, chunks,
    block_seq_in, block_pos_in, lengths_in, slopes_in, query, keys, values, weight,
    out,
    block_seq, block_pos, lengths, slopes,
    q_all, k_buf, v_buf, w_buf, stats, accs, held, part, landed,
    small_sem, q_sem, k_sem, v_sem, w_sem,
    q_send, q_recv, s_send, s_recv, a_send, a_recv, p_send, p_recv,
):
    me = lax.axis_index("seq")
    my_rows = lax.axis_index("tensor")
    blocks, block_len, features = k_buf.shape
    heads = slopes.shape[0]
    size = features // heads
    seqs = lengths.shape[0]
    query_rows = q_all.shape[1]
    rows, width = part.shape[2:]
    scale = 1.0 / math.sqrt(size)

    barrier = pltpu.get_barrier_semaphore()
    for k in range(1, seq_size):
        pl.semaphore_signal(barrier, inc=1, device_id={"seq": lax.rem(me + k, seq_size)})
    for k in range(1, tensor_size):
        pl.semaphore_signal(
            barrier, inc=1, device_id={"tensor": lax.rem(my_rows + k, tensor_size)}
        )
    q_copy = pltpu.make_async_copy(query, q_all.at[me], q_sem)
    q_copy.start()
    small_copies = [
        pltpu.make_async_copy(source, target, small_sem.at[i])
        for i, (source, target) in enumerate(
            [
                (block_seq_in, block_seq),
                (block_pos_in, block_pos),
                (lengths_in, lengths),
                (slopes_in, slopes),
            ]
        )
    ]
    for copy in small_copies:
        copy.start()
    cache_copies = [
        pltpu.make_async_copy(cache.at[b], buffer.at[b], sem.at[b])
        for cache, buffer, sem in ((keys, k_buf, k_sem), (values, v_buf, v_sem))
        for b in range(blocks)
    ]
    spans = [(first * size, last * size) for first, last in groups]
    w_copies = [
        pltpu.make_async_copy(
            weight.at[pl.ds(low, high - low)], w_buf.at[pl.ds(low, high - low)], w_sem.at[g]
        )
        for g, (low, high) in enumerate(spans)
    ]

    q_copy.wait()
    for copy in cache_copies:
        copy.start()
    pl.semaphore_wait(barrier, seq_size + tensor_size - 2)

    def to_seq(buffer, send, recv):
        copies = [
            pltpu.make_async_remote_copy(
                src_ref=buffer.at[me],
                dst_ref=buffer.at[me],
                send_sem=send.at[k - 1],
                recv_sem=recv.at[k - 1],
                device_id={"seq": lax.rem(me + k, seq_size)},
            )
            for k in range(1, seq_size)
        ]
        for copy in copies:
            copy.start()
        return copies

    q_sends = to_seq(q_all, q_send, q_recv)

    for copy in small_copies:
        copy.wait()
    offsets = lax.broadcasted_iota(jnp.int32, (1, block_len), 1)
    stat_lane = lax.broadcasted_iota(jnp.int32, (1, LANES), 1)

    for copy in q_sends:
        copy.wait_recv()
    for copy in w_copies:
        copy.start()
    for copy in cache_copies:
        copy.wait()

    q_rows = []
    for b in range(blocks):
        owner = block_seq[b]
        near = q_all[lax.div(owner, query_rows)].astype(jnp.float32)
        which = lax.rem(owner, query_rows)
        q_row = near[:1]
        for r in range(1, query_rows):
            q_row = jnp.where(which == r, near[r : r + 1], q_row)
        q_rows.append(q_row)

    s_sends, a_sends = [], []
    for g, (first, last) in enumerate(groups):
        low, high = spans[g]
        padded = -(-(last - first) // 16) * 16
        lane = lax.broadcasted_iota(jnp.int32, (padded, high - low), 1)
        row = lax.broadcasted_iota(jnp.int32, (padded, high - low), 0)
        of_head = (lane >= row * size) & (lane < row * size + size)
        head_row = lax.broadcasted_iota(jnp.int32, (padded, LANES), 0)
        head_lane = lax.broadcasted_iota(jnp.int32, (padded, LANES), 1)
        slope = jnp.zeros((padded, LANES), jnp.float32)
        for h in range(first, last):
            slope = jnp.where(head_row == h - first, slopes[h], slope)
        slope = slope[:, :1]
        weights, inverse, stat_rows = [], [], []
        for b in range(blocks):
            owner = block_seq[b]
            length = lengths[owner]
            spread = jnp.where(of_head, q_rows[b][:, low:high], 0.0).astype(jnp.bfloat16)
            scores = lax.dot_general(
                spread,
                k_buf[b, :, low:high],
                (((1,), (1,)), ((), ())),
                preferred_element_type=jnp.float32,
            )
            placed = block_pos[b] * block_len + offsets
            live = placed < length
            distance = (length - 1 - placed).astype(jnp.float32)
            scores = jnp.where(live, scores * scale - slope * distance, -1e30)
            top = jnp.max(scores, axis=1, keepdims=True)
            weight_b = jnp.where(live, jnp.exp(scores - top), 0.0)
            total = jnp.sum(weight_b, axis=1, keepdims=True)
            weights.append(weight_b.astype(jnp.bfloat16))
            inverse.append(1.0 / total)
            stat = jnp.sum(
                jnp.where(head_row == head_lane, top + jnp.log(total), 0.0), axis=0, keepdims=True
            )
            stat_rows.append(jnp.where(stat_lane == OWNER_LANE, owner.astype(jnp.float32), stat))
        stats[g][me] = jnp.concatenate(stat_rows, axis=0)
        s_sends.append(to_seq(stats[g], s_send.at[g], s_recv.at[g]))
        acc_rows = []
        for b in range(blocks):
            summed = jnp.dot(
                weights[b], v_buf[b, :, low:high], preferred_element_type=jnp.float32
            )
            summed = summed * inverse[b]
            acc_rows.append(jnp.sum(jnp.where(of_head, summed, 0.0), axis=0, keepdims=True))
        accs[g][me] = jnp.concatenate(acc_rows, axis=0).astype(jnp.bfloat16)
        a_sends.append(to_seq(accs[g], a_send.at[g], a_recv.at[g]))

    def attention_of(g):
        for copy in s_sends[g]:
            copy.wait_recv()
        stat = stats[g][...]
        owners = stat[:, :, OWNER_LANE:]
        best = jnp.zeros_like(stat)
        masks = [owners == float(s) for s in range(seqs)]
        for s in range(seqs):
            top = jnp.max(jnp.where(masks[s], stat, -1e30), axis=(0, 1), keepdims=True)
            best = jnp.where(masks[s], top, best)
        grown = jnp.exp(stat - best)
        whole = jnp.ones_like(stat)
        for s in range(seqs):
            total = jnp.sum(jnp.where(masks[s], grown, 0.0), axis=(0, 1), keepdims=True)
            whole = jnp.where(masks[s], total, whole)
        factor = grown / whole
        seq_lane = lax.broadcasted_iota(jnp.int32, (blocks, LANES), 1).astype(jnp.float32)
        owned = jnp.concatenate(
            [jnp.where(owners[j] == seq_lane, 1.0, 0.0) for j in range(seq_size)], axis=0
        )
        owned = owned.T[:seqs].astype(jnp.bfloat16)
        first, last = groups[g]
        spread = [
            jnp.concatenate(
                [
                    jnp.broadcast_to(factor[j][:, h : h + 1], (blocks, size))
                    for h in range(last - first)
                ],
                axis=1,
            )
            for j in range(seq_size)
        ]
        for copy in a_sends[g]:
            copy.wait_recv()
        w_copies[g].wait()
        scaled = jnp.concatenate(
            [accs[g][j].astype(jnp.float32) * spread[j] for j in range(seq_size)], axis=0
        )
        upper = scaled.astype(jnp.bfloat16)
        lower = (scaled - upper.astype(jnp.float32)).astype(jnp.bfloat16)
        attention = jnp.dot(owned, upper, preferred_element_type=jnp.float32) + jnp.dot(
            owned, lower, preferred_element_type=jnp.float32
        )
        return attention.astype(jnp.bfloat16)

    for g, (low, high) in enumerate(spans[:-1]):
        attention = attention_of(g)
        product = jnp.dot(attention, w_buf[low:high], preferred_element_type=jnp.float32)
        held[...] = product if g == 0 else held[...] + product
    attention = attention_of(len(groups) - 1)
    low, high = spans[-1]

    p_sends = []
    for c in range(chunks):
        columns = slice(c * width, (c + 1) * width)
        product = jnp.dot(attention, w_buf[low:high, columns], preferred_element_type=jnp.float32)
        product = product + held[:, columns]
        for r in range(tensor_size):
            part[r, c] = product[r * rows : (r + 1) * rows]
        sends = []
        for k in range(1, tensor_size):
            peer = lax.rem(my_rows + k, tensor_size)
            copy = pltpu.make_async_remote_copy(
                src_ref=part.at[peer, c],
                dst_ref=landed.at[k - 1, c],
                send_sem=p_send.at[k - 1, c],
                recv_sem=p_recv.at[k - 1, c],
                device_id={"tensor": peer},
            )
            copy.start()
            sends.append(copy)
        p_sends.append(sends)
    for c in range(chunks):
        total = part[my_rows, c]
        for k in range(1, tensor_size):
            p_sends[c][k - 1].wait_recv()
            total = total + landed[k - 1, c]
        out[:, c * width : (c + 1) * width] = total.astype(out.dtype)
    for sends in [q_sends] + s_sends + a_sends + p_sends:
        for copy in sends:
            copy.wait_send()


def local(seq_size, tensor_size, query, key_cache, value_cache, slopes, block_seq, block_pos, lengths, weight):
    heads = slopes.shape[0]
    blocks, block_len, features = key_cache.shape
    size = features // heads
    columns = weight.shape[1]
    chunks = max([c for c in range(1, 9) if columns % (c * 256) == 0], default=1)
    width = columns // chunks
    rows = lengths.shape[0] // tensor_size
    middle = min(heads, -(-heads // 4) * 2)
    groups = [(low, high) for low, high in ((0, middle), (middle, heads)) if high > low]
    smalls = (block_seq, block_pos, lengths, slopes)
    dma = pltpu.SemaphoreType.DMA
    return pl.pallas_call(
        functools.partial(kernel, seq_size, tensor_size, groups, chunks),
        out_shape=pltpu.VMEM((rows, columns), jnp.bfloat16),
        in_specs=[pl.BlockSpec(memory_space=pltpu.HBM)] * 8,
        out_specs=pl.BlockSpec(memory_space=pltpu.VMEM),
        scratch_shapes=[pltpu.SMEM(a.shape, a.dtype) for a in smalls]
        + [
            pltpu.VMEM((seq_size,) + query.shape, query.dtype),
            pltpu.VMEM(key_cache.shape, key_cache.dtype),
            pltpu.VMEM(value_cache.shape, value_cache.dtype),
            pltpu.VMEM(weight.shape, weight.dtype),
            [pltpu.VMEM((seq_size, blocks, LANES), jnp.float32) for _ in groups],
            [
                pltpu.VMEM((seq_size, blocks, (high - low) * size), jnp.bfloat16)
                for low, high in groups
            ],
            pltpu.VMEM((lengths.shape[0], columns), jnp.float32),
            pltpu.VMEM((tensor_size, chunks, rows, width), jnp.float32),
            pltpu.VMEM((tensor_size - 1, chunks, rows, width), jnp.float32),
            dma((4,)),
            dma,
            dma((blocks,)),
            dma((blocks,)),
            dma((len(groups),)),
        ]
        + [dma((seq_size - 1,))] * 2
        + [dma((len(groups), seq_size - 1))] * 4
        + [dma((tensor_size - 1, chunks))] * 2,
        compiler_params=pltpu.CompilerParams(
            collective_id=0, has_side_effects=True, vmem_limit_bytes=48 * 1024 * 1024
        ),
    )(
        *[
            pltpu.with_memory_space_constraint(a, pltpu.HBM)
            for a in smalls + (query, key_cache, value_cache, weight)
        ]
    )


def solution(mesh):
    placed = (
        P(("group", "seq"), "tensor"),
        P(("group", "seq"), None, "tensor"),
        P(("group", "seq"), None, "tensor"),
        P("tensor"),
        P(("group", "seq")),
        P(("group", "seq")),
        P("group"),
        P("tensor", "seq"),
    )
    return jax.shard_map(
        functools.partial(local, mesh.shape["seq"], mesh.shape["tensor"]),
        mesh=mesh,
        in_specs=placed,
        out_specs=P(("group", "tensor"), "seq"),
        check_vma=False,
    )
```

```python
import functools
import math

import jax
import jax.numpy as jnp
from jax import lax
from jax.experimental import pallas as pl
from jax.experimental.pallas import tpu as pltpu
from jax.sharding import PartitionSpec as P

LANES = 128
OWNER_LANE = LANES - 1


def kernel(
    seq_size, tensor_size, groups, chunks,
    block_seq_in, block_pos_in, lengths_in, slopes_in, query, keys, values, weight,
    out,
    block_seq, block_pos, lengths, slopes,
    q_all, k_buf, v_buf, w_buf, stats, accs, held, part, landed,
    small_sem, q_sem, k_sem, v_sem, w_sem,
    q_send, q_recv, s_send, s_recv, a_send, a_recv, p_send, p_recv,
):
    me = lax.axis_index("seq")
    my_rows = lax.axis_index("tensor")
    blocks, block_len, features = k_buf.shape
    heads = slopes.shape[0]
    size = features // heads
    seqs = lengths.shape[0]
    query_rows = q_all.shape[1]
    rows, width = part.shape[2:]
    scale = 1.0 / math.sqrt(size)

    barrier = pltpu.get_barrier_semaphore()
    for k in range(1, seq_size):
        pl.semaphore_signal(barrier, inc=1, device_id={"seq": lax.rem(me + k, seq_size)})
    for k in range(1, tensor_size):
        pl.semaphore_signal(
            barrier, inc=1, device_id={"tensor": lax.rem(my_rows + k, tensor_size)}
        )
    q_copy = pltpu.make_async_copy(query, q_all.at[me], q_sem)
    q_copy.start()
    small_copies = [
        pltpu.make_async_copy(source, target, small_sem.at[i])
        for i, (source, target) in enumerate(
            [
                (block_seq_in, block_seq),
                (block_pos_in, block_pos),
                (lengths_in, lengths),
                (slopes_in, slopes),
            ]
        )
    ]
    for copy in small_copies:
        copy.start()
    cache_copies = [
        pltpu.make_async_copy(cache.at[b], buffer.at[b], sem.at[b])
        for cache, buffer, sem in ((keys, k_buf, k_sem), (values, v_buf, v_sem))
        for b in range(blocks)
    ]
    spans = [(first * size, last * size) for first, last in groups]
    w_copies = [
        pltpu.make_async_copy(
            weight.at[pl.ds(low, high - low)], w_buf.at[pl.ds(low, high - low)], w_sem.at[g]
        )
        for g, (low, high) in enumerate(spans)
    ]

    q_copy.wait()
    for copy in cache_copies:
        copy.start()
    pl.semaphore_wait(barrier, seq_size + tensor_size - 2)

    def to_seq(buffer, send, recv):
        copies = [
            pltpu.make_async_remote_copy(
                src_ref=buffer.at[me],
                dst_ref=buffer.at[me],
                send_sem=send.at[k - 1],
                recv_sem=recv.at[k - 1],
                device_id={"seq": lax.rem(me + k, seq_size)},
            )
            for k in range(1, seq_size)
        ]
        for copy in copies:
            copy.start()
        return copies

    q_sends = to_seq(q_all, q_send, q_recv)

    for copy in small_copies:
        copy.wait()
    offsets = lax.broadcasted_iota(jnp.int32, (1, block_len), 1)
    stat_lane = lax.broadcasted_iota(jnp.int32, (1, LANES), 1)

    for copy in q_sends:
        copy.wait_recv()
    for copy in w_copies:
        copy.start()
    for copy in cache_copies:
        copy.wait()

    q_rows = []
    for b in range(blocks):
        owner = block_seq[b]
        near = q_all[lax.div(owner, query_rows)].astype(jnp.float32)
        which = lax.rem(owner, query_rows)
        q_row = near[:1]
        for r in range(1, query_rows):
            q_row = jnp.where(which == r, near[r : r + 1], q_row)
        q_rows.append(q_row)

    s_sends, a_sends = [], []
    for g, (first, last) in enumerate(groups):
        low, high = spans[g]
        padded = -(-(last - first) // 16) * 16
        lane = lax.broadcasted_iota(jnp.int32, (padded, high - low), 1)
        row = lax.broadcasted_iota(jnp.int32, (padded, high - low), 0)
        of_head = (lane >= row * size) & (lane < row * size + size)
        head_row = lax.broadcasted_iota(jnp.int32, (padded, LANES), 0)
        head_lane = lax.broadcasted_iota(jnp.int32, (padded, LANES), 1)
        slope = jnp.zeros((padded, LANES), jnp.float32)
        for h in range(first, last):
            slope = jnp.where(head_row == h - first, slopes[h], slope)
        slope = slope[:, :1]
        weights, inverse, stat_rows = [], [], []
        for b in range(blocks):
            owner = block_seq[b]
            length = lengths[owner]
            spread = jnp.where(of_head, q_rows[b][:, low:high], 0.0).astype(jnp.bfloat16)
            scores = lax.dot_general(
                spread,
                k_buf[b, :, low:high],
                (((1,), (1,)), ((), ())),
                preferred_element_type=jnp.float32,
            )
            placed = block_pos[b] * block_len + offsets
            live = placed < length
            distance = (length - 1 - placed).astype(jnp.float32)
            scores = jnp.where(live, scores * scale - slope * distance, -1e30)
            top = jnp.max(scores, axis=1, keepdims=True)
            weight_b = jnp.where(live, jnp.exp(scores - top), 0.0)
            total = jnp.sum(weight_b, axis=1, keepdims=True)
            weights.append(weight_b.astype(jnp.bfloat16))
            inverse.append(1.0 / total)
            stat = jnp.sum(
                jnp.where(head_row == head_lane, top + jnp.log(total), 0.0), axis=0, keepdims=True
            )
            stat_rows.append(jnp.where(stat_lane == OWNER_LANE, owner.astype(jnp.float32), stat))
        stats[g][me] = jnp.concatenate(stat_rows, axis=0)
        s_sends.append(to_seq(stats[g], s_send.at[g], s_recv.at[g]))
        acc_rows = []
        for b in range(blocks):
            summed = jnp.dot(
                weights[b], v_buf[b, :, low:high], preferred_element_type=jnp.float32
            )
            summed = summed * inverse[b]
            acc_rows.append(jnp.sum(jnp.where(of_head, summed, 0.0), axis=0, keepdims=True))
        accs[g][me] = jnp.concatenate(acc_rows, axis=0).astype(jnp.bfloat16)
        a_sends.append(to_seq(accs[g], a_send.at[g], a_recv.at[g]))

    def attention_of(g):
        for copy in s_sends[g]:
            copy.wait_recv()
        stat = stats[g][...]
        owners = stat[:, :, OWNER_LANE:]
        best = jnp.zeros_like(stat)
        masks = [owners == float(s) for s in range(seqs)]
        for s in range(seqs):
            top = jnp.max(jnp.where(masks[s], stat, -1e30), axis=(0, 1), keepdims=True)
            best = jnp.where(masks[s], top, best)
        grown = jnp.exp(stat - best)
        whole = jnp.ones_like(stat)
        for s in range(seqs):
            total = jnp.sum(jnp.where(masks[s], grown, 0.0), axis=(0, 1), keepdims=True)
            whole = jnp.where(masks[s], total, whole)
        factor = grown / whole
        seq_lane = lax.broadcasted_iota(jnp.int32, (blocks, LANES), 1).astype(jnp.float32)
        owned = jnp.concatenate(
            [jnp.where(owners[j] == seq_lane, 1.0, 0.0) for j in range(seq_size)], axis=0
        )
        owned = owned.T[:seqs].astype(jnp.bfloat16)
        first, last = groups[g]
        spread = [
            jnp.concatenate(
                [
                    jnp.broadcast_to(factor[j][:, h : h + 1], (blocks, size))
                    for h in range(last - first)
                ],
                axis=1,
            )
            for j in range(seq_size)
        ]
        for copy in a_sends[g]:
            copy.wait_recv()
        w_copies[g].wait()
        scaled = jnp.concatenate(
            [accs[g][j].astype(jnp.float32) * spread[j] for j in range(seq_size)], axis=0
        )
        upper = scaled.astype(jnp.bfloat16)
        lower = (scaled - upper.astype(jnp.float32)).astype(jnp.bfloat16)
        attention = jnp.dot(owned, upper, preferred_element_type=jnp.float32) + jnp.dot(
            owned, lower, preferred_element_type=jnp.float32
        )
        return attention.astype(jnp.bfloat16)

    for g, (low, high) in enumerate(spans[:-1]):
        attention = attention_of(g)
        product = jnp.dot(attention, w_buf[low:high], preferred_element_type=jnp.float32)
        held[...] = product if g == 0 else held[...] + product
    attention = attention_of(len(groups) - 1)
    low, high = spans[-1]

    p_sends = []

    def product_of(c):
        columns = slice(c * width, (c + 1) * width)
        product = jnp.dot(attention, w_buf[low:high, columns], preferred_element_type=jnp.float32)
        return product + held[:, columns]

    later = product_of(0)
    for c in range(chunks):
        product = later
        if c + 1 < chunks:
            later = product_of(c + 1)
        for r in range(tensor_size):
            part[r, c] = product[r * rows : (r + 1) * rows]
        sends = []
        for k in range(1, tensor_size):
            peer = lax.rem(my_rows + k, tensor_size)
            copy = pltpu.make_async_remote_copy(
                src_ref=part.at[peer, c],
                dst_ref=landed.at[k - 1, c],
                send_sem=p_send.at[k - 1, c],
                recv_sem=p_recv.at[k - 1, c],
                device_id={"tensor": peer},
            )
            copy.start()
            sends.append(copy)
        p_sends.append(sends)
    for c in range(chunks):
        total = part[my_rows, c]
        for k in range(1, tensor_size):
            p_sends[c][k - 1].wait_recv()
            total = total + landed[k - 1, c]
        out[:, c * width : (c + 1) * width] = total.astype(out.dtype)
    for sends in [q_sends] + s_sends + a_sends + p_sends:
        for copy in sends:
            copy.wait_send()


def local(seq_size, tensor_size, query, key_cache, value_cache, slopes, block_seq, block_pos, lengths, weight):
    heads = slopes.shape[0]
    blocks, block_len, features = key_cache.shape
    size = features // heads
    columns = weight.shape[1]
    chunks = max([c for c in range(1, 9) if columns % (c * 256) == 0], default=1)
    width = columns // chunks
    rows = lengths.shape[0] // tensor_size
    middle = min(heads, -(-heads // 4) * 2)
    groups = [(low, high) for low, high in ((0, middle), (middle, heads)) if high > low]
    smalls = (block_seq, block_pos, lengths, slopes)
    dma = pltpu.SemaphoreType.DMA
    return pl.pallas_call(
        functools.partial(kernel, seq_size, tensor_size, groups, chunks),
        out_shape=pltpu.VMEM((rows, columns), jnp.bfloat16),
        in_specs=[pl.BlockSpec(memory_space=pltpu.HBM)] * 8,
        out_specs=pl.BlockSpec(memory_space=pltpu.VMEM),
        scratch_shapes=[pltpu.SMEM(a.shape, a.dtype) for a in smalls]
        + [
            pltpu.VMEM((seq_size,) + query.shape, query.dtype),
            pltpu.VMEM(key_cache.shape, key_cache.dtype),
            pltpu.VMEM(value_cache.shape, value_cache.dtype),
            pltpu.VMEM(weight.shape, weight.dtype),
            [pltpu.VMEM((seq_size, blocks, LANES), jnp.float32) for _ in groups],
            [
                pltpu.VMEM((seq_size, blocks, (high - low) * size), jnp.bfloat16)
                for low, high in groups
            ],
            pltpu.VMEM((lengths.shape[0], columns), jnp.float32),
            pltpu.VMEM((tensor_size, chunks, rows, width), jnp.float32),
            pltpu.VMEM((tensor_size - 1, chunks, rows, width), jnp.float32),
            dma((4,)),
            dma,
            dma((blocks,)),
            dma((blocks,)),
            dma((len(groups),)),
        ]
        + [dma((seq_size - 1,))] * 2
        + [dma((len(groups), seq_size - 1))] * 4
        + [dma((tensor_size - 1, chunks))] * 2,
        compiler_params=pltpu.CompilerParams(
            collective_id=0, has_side_effects=True, vmem_limit_bytes=48 * 1024 * 1024
        ),
    )(
        *[
            pltpu.with_memory_space_constraint(a, pltpu.HBM)
            for a in smalls + (query, key_cache, value_cache, weight)
        ]
    )


def solution(mesh):
    placed = (
        P(("group", "seq"), "tensor"),
        P(("group", "seq"), None, "tensor"),
        P(("group", "seq"), None, "tensor"),
        P("tensor"),
        P(("group", "seq")),
        P(("group", "seq")),
        P("group"),
        P("tensor", "seq"),
    )
    return jax.shard_map(
        functools.partial(local, mesh.shape["seq"], mesh.shape["tensor"]),
        mesh=mesh,
        in_specs=placed,
        out_specs=P(("group", "tensor"), "seq"),
        check_vma=False,
    )
```
